256 devices in a mesh: rep: 4 (over x_hi, core), fsdp: 64 (over x_lo, z, y).
Axes of the slice: x: 4 (x_hi: 2, x_lo: 2; x = x_hi * 2 + x_lo), y: 4, z: 8, core: 2. Of those that a mesh axis runs over, the one named last changes fastest.
Arguments:
- layer_inputs: bfloat16 [65536, 4608], P(('rep', 'fsdp')), may hold values from -24 to 24
- queries: bfloat16 [65536, 2048], P(('rep', 'fsdp')), may hold values from -32 to 32
- saved_keys: bfloat16 [65536, 1024], P(('rep', 'fsdp')), may hold values from -6 to 6
- saved_values: bfloat16 [65536, 1024], P(('rep', 'fsdp')), may hold values from -6 to 6
- out_grad: bfloat16 [65536, 2048], P(('rep', 'fsdp')), may hold values from -0.625 to 0.625
- global_params: float32 [4608, 1024], P('fsdp'), may hold values from -0.09375 to 0.09375
- replica_params: float32 [4, 4608, 1024], P('rep', 'fsdp'), may hold values from -0.09375 to 0.09375
- outer_momentum: float32 [4608, 1024], P('fsdp'), may hold values from -0.125 to 0.125
- next_inputs: bfloat16 [65536, 4608], P(('rep', 'fsdp')), may hold values from -6 to 6
Outputs:
- new_params: float32 [4608, 1024], P('fsdp')
- new_momentum: float32 [4608, 1024], P('fsdp')
- next_keys: bfloat16 [65536, 1024], P(('rep', 'fsdp'))
The draws below stay inside these ranges and needn't reach their ends.
All inputs are finite; a program needn't handle non-finite values.
Results may differ from the reference program's by a relative error of at most 0.014.
Values may be sent and summed in bfloat16 or wider, within the bound.
No kernel may reach another device: no remote copies, remote signals or barrier semaphores. Data moves between devices by JAX's collectives and lax.ppermute only.
A program may use at most 128 MiB of HBM per device.

```python
import jax
import jax.numpy as jnp
from jax import lax

D = 4608
QH = 16
KVH = 8
HD = 128
SEQ_LEN = 256
TOKENS = 65536
N_REP = 4
N_FSDP = 64


def spiked(array, stream_key, source, target, blocks, factor):
    owner, partner = [(jnp.arange(array.shape[position]) // (array.shape[position] // blocks)).reshape([-1 if axis == position else 1 for axis in range(array.ndim)]) for position in (source, target)]
    chosen = jax.random.permutation(stream_key, blocks)[partner]
    strong = (owner == chosen) | (owner == (partner + blocks // 2) % blocks)
    return jnp.where(strong, factor * array, array)


def shard_levels(rng, dims, shards, low, top_value):
    def one(position, parts):
        heights = jax.random.uniform(jax.random.fold_in(jax.random.fold_in(rng, 6), position), (parts,), jnp.float32, low / len(shards), top_value / len(shards))
        return jnp.repeat(jnp.exp(heights), dims[position] // parts).reshape((-1,) + (1,) * (len(dims) - position - 1))

    factor_of = one(*shards[0])
    for cut in shards[1:]:
        factor_of = factor_of * one(*cut)
    return factor_of


def centred(stream_key, shape, width, reach, cuts=(), dtype=jnp.bfloat16):
    loudness = shard_levels(stream_key, shape, cuts, -0.22, 0.18) if cuts else 1.0
    drawn = jax.random.normal(stream_key, shape, jnp.float32) * width * loudness
    return jnp.minimum(jnp.maximum(drawn, -reach), reach).astype(dtype)


def gaussian_with(rng, extent, deviation, reach, cuts, heavy, kind=jnp.bfloat16):
    drawn = deviation * jax.random.normal(rng, extent, jnp.float32)
    if cuts:
        drawn = drawn * shard_levels(rng, extent, cuts, -0.22, 0.18)
    return jnp.clip(spiked(drawn, jax.random.fold_in(rng, 3), *heavy), -reach, reach).astype(kind)


def setup_inputs(seed: int = 0) -> dict:
    streams_of = jax.random.split(jax.random.key(seed), 10)
    return {
        "layer_inputs": gaussian_with(streams_of[0], (TOKENS, D), 1.0, 24.0, ((0, 256),), (0, 1, 256, 6.0)),
        "queries": centred(streams_of[1], (TOKENS, QH * HD), 5.0, 32.0, ((0, 256),)),
        "saved_keys": centred(streams_of[2], (TOKENS, KVH * HD), 1.0, 6.0, ((0, 256),)),
        "saved_values": centred(streams_of[3], (TOKENS, KVH * HD), 1.0, 6.0, ((0, 256),)),
        "out_grad": centred(streams_of[4], (TOKENS, QH * HD), 0.1, 0.625, ((0, 256),)),
        "global_params": centred(streams_of[5], (D, KVH * HD), D ** -0.5, 0.09375, ((0, 64),), jnp.float32),
        "replica_params": centred(streams_of[6], (N_REP, D, KVH * HD), D ** -0.5, 0.09375, ((0, 4), (1, 64)), jnp.float32),
        "outer_momentum": centred(streams_of[7], (D, KVH * HD), 0.02, 0.125, ((0, 64),), jnp.float32),
        "next_inputs": centred(streams_of[8], (TOKENS, D), 1.0, 6.0, ((0, 256),)),
    }


score_scale = 1.0 / 12.0
soft_cap = 50.0
rope_base = 10000.0
inner_rate = 0.02
outer_rate = 0.7
outer_beta = 0.9


def rotate_back(grads, length):
    half = grads.shape[-1] // 2
    places = jnp.arange(length).astype(jnp.float32)
    freqs = rope_base ** (-jnp.arange(half).astype(jnp.float32) / half)
    angles = (places[:, None] * freqs[None, :])[:, None, :]
    cosine = jnp.cos(angles)
    sine = jnp.sin(angles)
    first = grads[..., :half]
    second = grads[..., half:]
    return jnp.concatenate([first * cosine + second * sine, second * cosine - first * sine], axis=-1)


def attention_keys(query_rows, key_rows, value_rows, grad_rows):
    length = query_rows.shape[0]
    group = QH // KVH
    query_wide = query_rows.astype(jnp.float32).reshape(length, KVH, group, HD)
    key_wide = key_rows.astype(jnp.float32).reshape(length, KVH, HD)
    value_wide = value_rows.astype(jnp.float32).reshape(length, KVH, HD)
    grad_wide = grad_rows.astype(jnp.float32).reshape(length, KVH, group, HD)
    logits = jnp.einsum("ihgd,jhd->hgij", query_wide, key_wide) * score_scale
    capped = jnp.tanh(logits / soft_cap)
    row_index = jnp.arange(length)
    causal = row_index[:, None] >= row_index[None, :]
    unnormed = jnp.where(causal, jnp.exp(soft_cap * capped), jnp.float32(0.0))
    probs = unnormed / jnp.sum(unnormed, axis=-1, keepdims=True)
    dprobs = jnp.einsum("ihgd,jhd->hgij", grad_wide, value_wide)
    center = jnp.sum(probs * dprobs, axis=-1, keepdims=True)
    dlogits = (probs * (dprobs - center) * (1.0 - capped * capped) * score_scale).astype(jnp.bfloat16)
    rotated = jnp.einsum("hgij,ihgd->jhd", dlogits.astype(jnp.float32), query_wide)
    plain = rotate_back(rotated, length)
    return plain.reshape(length, KVH * HD).astype(jnp.bfloat16)


def reference(layer_inputs, queries, saved_keys, saved_values, out_grad, global_params, replica_params, outer_momentum, next_inputs):
    seqs = N_REP * N_FSDP
    packed = (queries.reshape(seqs, SEQ_LEN, QH * HD), saved_keys.reshape(seqs, SEQ_LEN, KVH * HD),
              saved_values.reshape(seqs, SEQ_LEN, KVH * HD), out_grad.reshape(seqs, SEQ_LEN, QH * HD))
    key_grads = lax.map(lambda member: attention_keys(member[0], member[1], member[2], member[3]), packed)
    key_grads = key_grads.reshape(seqs * SEQ_LEN, KVH * HD)
    group_tokens = N_FSDP * SEQ_LEN
    summed = jnp.zeros(global_params.shape, jnp.float32)
    for replica in range(N_REP):
        token_rows = layer_inputs[replica * group_tokens:(replica + 1) * group_tokens]
        grad_rows = key_grads[replica * group_tokens:(replica + 1) * group_tokens]
        group_grad = jnp.dot(token_rows.T, grad_rows, preferred_element_type=jnp.float32)
        finished = replica_params[replica] - inner_rate * group_grad
        summed = summed + (global_params - finished)
    outer_grad = summed / N_REP
    new_momentum = outer_beta * outer_momentum + outer_grad
    new_params = global_params - outer_rate * (outer_grad + outer_beta * new_momentum)
    next_keys = jnp.dot(next_inputs, new_params.astype(jnp.bfloat16), preferred_element_type=jnp.float32).astype(jnp.bfloat16)
    return new_params, new_momentum, next_keys
```

```python
import jax
import jax.numpy as jnp
from jax import lax
from jax.sharding import Mesh
from jax.sharding import PartitionSpec as P

QH = 16
KVH = 8
HD = 128
AXES = ("xh", "core", "xl", "z", "y")
SIZES = (2, 2, 2, 8, 4)
FSDP = ("xl", "z", "y")
REP = ("xh", "core")
X = ("xh", "xl")

score_scale = 1.0 / 12.0
soft_cap = 50.0
rope_base = 10000.0
inner_rate = 0.02
outer_rate = 0.7
outer_beta = 0.9


def place(xh, core, xl, z, y):
    return (((xh * 2 + core) * 2 + xl) * 8 + z) * 4 + y


def every_device():
    for xh in range(2):
        for core in range(2):
            for xl in range(2):
                for z in range(8):
                    for y in range(4):
                        yield xh, core, xl, z, y


def owner_routes():
    first, second = [], []
    for xh, core, xl, z, y in every_device():
        block = (xl * 8 + z) * 4 + y
        high, mid, low = block // 16, (block // 4) % 4, block % 4
        source = place(xh, core, xl, z, y)
        first.append((source, place(high // 2, core, high % 2, xh * 4 + low, mid)))
        second.append((source, place(mid // 2, core, mid % 2, xh * 4 + low, high)))
    return first, second


def send(value, route):
    return lax.ppermute(value, AXES, route)


def other_core(value):
    return send(value, [(place(xh, c, xl, z, y), place(xh, 1 - c, xl, z, y)) for xh, c, xl, z, y in every_device()])


def swap(blocks, axes):
    return lax.all_to_all(blocks, axes, 0, 0, tiled=True)


def spread(value, axes, count):
    return swap(jnp.broadcast_to(value[None], (count, *value.shape)), axes)


def rotate_back(grads, length):
    half = grads.shape[-1] // 2
    places = jnp.arange(length).astype(jnp.float32)
    freqs = rope_base ** (-jnp.arange(half).astype(jnp.float32) / half)
    angles = (places[:, None] * freqs[None, :])[:, None, :]
    cosine = jnp.cos(angles)
    sine = jnp.sin(angles)
    first = grads[..., :half]
    second = grads[..., half:]
    return jnp.concatenate(
        [first * cosine + second * sine, second * cosine - first * sine], axis=-1
    )


def attention_keys(query_rows, key_rows, value_rows, grad_rows):
    length = query_rows.shape[0]
    group = QH // KVH
    query_wide = query_rows.reshape(length, KVH, group, HD)
    key_wide = key_rows.reshape(length, KVH, HD)
    value_wide = value_rows.reshape(length, KVH, HD)
    grad_wide = grad_rows.reshape(length, KVH, group, HD)
    logits = (
        jnp.einsum("ihgd,jhd->hgij", query_wide, key_wide, preferred_element_type=jnp.float32)
        * score_scale
    )
    capped = jnp.tanh(logits / soft_cap)
    row_index = jnp.arange(length)
    causal = row_index[:, None] >= row_index[None, :]
    unnormed = jnp.where(causal, jnp.exp(soft_cap * capped), jnp.float32(0.0))
    probs = unnormed / jnp.sum(unnormed, axis=-1, keepdims=True)
    dprobs = jnp.einsum("ihgd,jhd->hgij", grad_wide, value_wide, preferred_element_type=jnp.float32)
    center = jnp.sum(probs * dprobs, axis=-1, keepdims=True)
    dlogits = (probs * (dprobs - center) * (1.0 - capped * capped) * score_scale).astype(
        jnp.bfloat16
    )
    rotated = jnp.einsum("hgij,ihgd->jhd", dlogits, query_wide, preferred_element_type=jnp.float32)
    plain = rotate_back(rotated, length)
    return plain.reshape(length, KVH * HD).astype(jnp.bfloat16)


def total(blocks):
    return jnp.sum(blocks.astype(jnp.float32), axis=0)


def body(
    layer_inputs,
    queries,
    saved_keys,
    saved_values,
    out_grad,
    global_params,
    replica_params,
    outer_momentum,
    next_inputs,
):
    low = jnp.bfloat16
    f32 = jnp.float32
    owner_a, owner_b = owner_routes()
    back_a = [(j, i) for i, j in owner_a]
    back_b = [(j, i) for i, j in owner_b]

    quarters = next_inputs.reshape(256, 4, 1152).transpose(1, 0, 2)
    next_x = swap(quarters, X).reshape(1024, 1152)
    next_y = swap(quarters, ("y",)).reshape(1024, 1152)
    other_x = other_core(next_x)
    other_y = other_core(next_y)
    other_inputs = other_core(layer_inputs)

    rep_mean = total(
        lax.all_gather(replica_params[0], REP)
    ) / 4.0
    drift = global_params - rep_mean
    base = global_params - outer_rate * (
        (1.0 + outer_beta) * drift + outer_beta * outer_beta * outer_momentum
    )
    col = (lax.axis_index("core") * 4 + lax.axis_index("xh")) * 128
    base_a = send(lax.dynamic_slice(base, (0, col), (72, 128)), owner_a)
    base_b = send(lax.dynamic_slice(base, (0, col + 256), (72, 128)), owner_b)

    key_grad = attention_keys(queries, saved_keys, saved_values, out_grad)
    core = lax.axis_index("core")
    own_half = lax.dynamic_slice(key_grad, (0, core * 512), (256, 512))
    other_half = other_core(lax.dynamic_slice(key_grad, (0, (1 - core) * 512), (256, 512)))
    rows = jnp.concatenate([layer_inputs, other_inputs], axis=0)
    grads = jnp.concatenate([own_half, other_half], axis=0)

    def product(columns):
        return lax.dot_general(
            rows, columns, (((0,), (0,)), ((), ())), preferred_element_type=f32
        ).astype(low)

    part_a = product(grads[:, :256]).reshape(4, 1152, 256)
    part_b = product(grads[:, 256:]).reshape(4, 1152, 256)
    sum_b = total(swap(part_b, ("y",))).astype(low).reshape(4, 288, 256)
    sum_a = total(swap(part_a, X)).astype(low).reshape(4, 288, 256)
    sum_a = total(swap(sum_a, ("y",))).astype(low)
    sum_b = total(swap(sum_b, X)).astype(low)

    def by_z(value):
        return value.reshape(4, 72, 2, 128).transpose(2, 0, 1, 3).reshape(8, 72, 128)

    both = jnp.stack([by_z(sum_a), by_z(sum_b)], axis=1)
    grad = total(swap(both, ("z",)))
    step = inner_rate / 4.0
    fresh = jnp.stack([base_a, base_b]) - (outer_rate * (1.0 + outer_beta) * step) * grad
    fresh = fresh.astype(low)
    wide = spread(fresh, ("z",), 8)

    def block(wide):
        return wide.reshape(2, 4, 72, 128).transpose(1, 2, 0, 3).reshape(288, 256)

    weights_a = spread(block(wide[:, 0]), ("y",), 4).reshape(1152, 256)
    weights_b = spread(block(wide[:, 1]), X, 4).reshape(1152, 256)

    def project(own, other, weights):
        first = jnp.dot(own, weights, preferred_element_type=f32).astype(low)
        second = jnp.dot(other, weights, preferred_element_type=f32).astype(low)
        return jnp.concatenate([first.reshape(4, 256, 256), second.reshape(4, 256, 256)], axis=1)

    out_a = total(swap(project(next_x, other_x, weights_a), X)).astype(low)
    out_b = total(swap(project(next_y, other_y, weights_b), ("y",))).astype(low)
    mine = jnp.concatenate([out_a[:256], out_b[:256]], axis=1)
    theirs = other_core(jnp.concatenate([out_a[256:], out_b[256:]], axis=1))
    next_keys = jnp.where(
        core == 0,
        jnp.concatenate([mine, theirs], axis=1),
        jnp.concatenate([theirs, mine], axis=1),
    )

    home = jnp.concatenate([send(grad[0], back_a), send(grad[1], back_b)], axis=1)
    homes = lax.all_gather(home, REP).reshape(2, 2, 72, 2, 128)
    full = homes.transpose(2, 1, 3, 0, 4).reshape(72, 1024)
    outer_grad = drift + step * full
    fresh_momentum = outer_beta * outer_momentum + outer_grad
    fresh_params = global_params - outer_rate * (outer_grad + outer_beta * fresh_momentum)
    return (fresh_params, fresh_momentum, next_keys)


def solution(mesh):
    finer = Mesh(mesh.devices.reshape(SIZES), AXES)
    everything = REP + FSDP
    return jax.shard_map(
        body,
        mesh=finer,
        in_specs=(
            P(everything, None),
            P(everything, None),
            P(everything, None),
            P(everything, None),
            P(everything, None),
            P(FSDP, None),
            P(REP, FSDP, None),
            P(FSDP, None),
            P(everything, None),
        ),
        out_specs=(P(FSDP, None), P(FSDP, None), P(everything, None)),
        check_vma=False,
    )
```

```python
import jax
import jax.numpy as jnp
from jax import lax
from jax.experimental import pallas as pl
from jax.experimental.pallas import tpu as pltpu
from jax.sharding import Mesh
from jax.sharding import PartitionSpec as P

QH = 16
KVH = 8
HD = 128
AXES = ("xh", "core", "xl", "z", "y")
SIZES = (2, 2, 2, 8, 4)
FSDP = ("xl", "z", "y")
REP = ("xh", "core")

score_scale = 1.0 / 12.0
soft_cap = 50.0
rope_base = 10000.0
inner_rate = 0.02
outer_rate = 0.7
outer_beta = 0.9


def place(xh, core, xl, z, y):
    return (((xh * 2 + core) * 2 + xl) * 8 + z) * 4 + y


def every_device():
    for xh in range(2):
        for core in range(2):
            for xl in range(2):
                for z in range(8):
                    for y in range(4):
                        yield xh, core, xl, z, y


def owner_routes():
    first, second = [], []
    for xh, core, xl, z, y in every_device():
        block = (xl * 8 + z) * 4 + y
        high, mid, low = block // 16, (block // 4) % 4, block % 4
        source = place(xh, core, xl, z, y)
        first.append((source, place(high // 2, core, high % 2, xh * 4 + low, mid)))
        second.append((source, place(mid // 2, core, mid % 2, xh * 4 + low, high)))
    return first, second


def send(value, route):
    return lax.ppermute(value, AXES, route)


def shifted(dx=0, dy=0, dcore=0, dxh=0):
    route = []
    for xh, core, xl, z, y in every_device():
        x = (xh * 2 + xl + dx + 2 * dxh) % 4
        route.append((place(xh, core, xl, z, y), place(x // 2, (core + dcore) % 2, x % 2, z, (y + dy) % 4)))
    return route


def other_core(value):
    return send(value, shifted(dcore=1))


def swap(blocks, axes):
    return lax.all_to_all(blocks, axes, 0, 0, tiled=True)


def spread(value, axes, count):
    return swap(jnp.broadcast_to(value[None], (count, *value.shape)), axes)


def x_index():
    return lax.axis_index("xh") * 2 + lax.axis_index("xl")


def picked(blocks, index):
    return lax.dynamic_index_in_dim(blocks, index, 0, keepdims=False)


def trade_x(blocks):
    x = x_index()
    moved = [send(picked(blocks, (x + k) % 4), shifted(dx=k)) for k in range(1, 4)]
    return [picked(blocks, x), *moved]


def trade_y(blocks):
    return swap(blocks, ("y",))


def gather_x(value):
    x = x_index()
    parts = [value, *(send(value, shifted(dx=k)) for k in range(1, 4))]
    return jnp.stack([lax.select_n((x - j) % 4, *parts) for j in range(4)])


def sum_list(parts):
    whole = parts[0].astype(jnp.float32)
    for part in parts[1:]:
        whole = whole + part.astype(jnp.float32)
    return whole


def rotate_back(grads, length):
    half = grads.shape[-1] // 2
    places = jnp.arange(length).astype(jnp.float32)
    freqs = rope_base ** (-jnp.arange(half).astype(jnp.float32) / half)
    angles = (places[:, None] * freqs[None, :])[:, None, :]
    cosine = jnp.cos(angles)
    sine = jnp.sin(angles)
    first = grads[..., :half]
    second = grads[..., half:]
    return jnp.concatenate(
        [first * cosine + second * sine, second * cosine - first * sine], axis=-1
    )


def attention_keys(query_rows, key_rows, value_rows, grad_rows):
    length = query_rows.shape[0]
    group = QH // KVH
    query_wide = query_rows.reshape(length, KVH, group, HD)
    key_wide = key_rows.reshape(length, KVH, HD)
    value_wide = value_rows.reshape(length, KVH, HD)
    grad_wide = grad_rows.reshape(length, KVH, group, HD)
    logits = (
        jnp.einsum("ihgd,jhd->hgij", query_wide, key_wide, preferred_element_type=jnp.float32)
        * score_scale
    )
    capped = jnp.tanh(logits / soft_cap)
    row_index = jnp.arange(length)
    causal = row_index[:, None] >= row_index[None, :]
    unnormed = jnp.where(causal, jnp.exp(soft_cap * capped), jnp.float32(0.0))
    probs = unnormed / jnp.sum(unnormed, axis=-1, keepdims=True)
    dprobs = jnp.einsum("ihgd,jhd->hgij", grad_wide, value_wide, preferred_element_type=jnp.float32)
    center = jnp.sum(probs * dprobs, axis=-1, keepdims=True)
    dlogits = (probs * (dprobs - center) * (1.0 - capped * capped) * score_scale).astype(
        jnp.bfloat16
    )
    rotated = jnp.einsum("hgij,ihgd->jhd", dlogits, query_wide, preferred_element_type=jnp.float32)
    plain = rotate_back(rotated, length)
    return plain.reshape(length, KVH * HD).astype(jnp.bfloat16)


def total(blocks):
    return jnp.sum(blocks.astype(jnp.float32), axis=0)


TOKEN_ROWS = (((0,), (0,)), ((), ()))


def together(*values):
    return lax.optimization_barrier(values)


def quarter_kernel(rows_ref, out_ref):
    out_ref[0] = rows_ref[...]


def column_quarters(rows):
    return pl.pallas_call(
        quarter_kernel,
        grid=(4,),
        in_specs=[pl.BlockSpec((256, 1152), lambda i: (0, i))],
        out_specs=pl.BlockSpec((1, 256, 1152), lambda i: (i, 0, 0)),
        out_shape=jax.ShapeDtypeStruct((4, 256, 1152), jnp.bfloat16),
        cost_estimate=pl.CostEstimate(flops=3_000_000, bytes_accessed=4_718_592, transcendentals=0),
        name="quarters",
    )(rows)


def product_kernel(own_ref, other_ref, grad_ref, other_grad_ref, a_ref, b_ref):
    whole = lax.dot_general(
        own_ref[...], grad_ref[...], TOKEN_ROWS, preferred_element_type=jnp.float32
    ) + lax.dot_general(
        other_ref[...], other_grad_ref[...], TOKEN_ROWS, preferred_element_type=jnp.float32
    )
    whole = whole.astype(jnp.bfloat16)
    a_ref[0] = whole[:, :256]
    b_ref[0] = whole[:, 256:]


def products(own, other, grad, other_grad):
    tall = 384
    inputs = pl.BlockSpec((256, tall), lambda i: (0, i))
    grads = pl.BlockSpec((256, 512), lambda i: (0, 0))
    out = pl.BlockSpec((1, tall, 256), lambda i: (i // 3, i % 3, 0))
    shape = jax.ShapeDtypeStruct((4, 1152, 256), jnp.bfloat16)
    return pl.pallas_call(
        product_kernel,
        grid=(12,),
        in_specs=[inputs, inputs, grads, grads],
        out_specs=[out, out],
        out_shape=[shape, shape],
        cost_estimate=pl.CostEstimate(flops=2_415_919_104, bytes_accessed=9_961_472, transcendentals=0),
        name="products",
    )(own, other, grad, other_grad)


def project_kernel(own_ref, other_ref, weights_ref, out_ref):
    weights = weights_ref[...]
    for k, ref in enumerate((own_ref, other_ref)):
        out_ref[0, k * 256 : (k + 1) * 256] = jnp.dot(
            ref[0], weights, preferred_element_type=jnp.float32
        ).astype(jnp.bfloat16)


def project(own, other, weights):
    rows = pl.BlockSpec((1, 256, 1152), lambda i: (i, 0, 0))
    return pl.pallas_call(
        project_kernel,
        grid=(4,),
        in_specs=[rows, rows, pl.BlockSpec((1152, 256), lambda i: (0, 0))],
        out_specs=pl.BlockSpec((1, 512, 256), lambda i: (i, 0, 0)),
        out_shape=jax.ShapeDtypeStruct((4, 512, 256), jnp.bfloat16),
        cost_estimate=pl.CostEstimate(flops=1_207_959_552, bytes_accessed=6_356_992, transcendentals=0),
        name="project",
    )(own, other, weights)


def body(
    layer_inputs,
    queries,
    saved_keys,
    saved_values,
    out_grad,
    global_params,
    replica_params,
    outer_momentum,
    next_inputs,
):
    low = jnp.bfloat16
    owner_a, owner_b = owner_routes()
    back_a = [(j, i) for i, j in owner_a]
    back_b = [(j, i) for i, j in owner_b]
    core = lax.axis_index("core")
    xh = lax.axis_index("xh")
    step = inner_rate / 4.0

    def half(value, index):
        return lax.dynamic_slice(value, (0, index * 512), (72, 512))

    def strips(value, index):
        return jnp.stack(
            [lax.dynamic_slice(value, (0, k * 256 + index * 128), (72, 128)) for k in range(2)]
        )

    quarters = column_quarters(next_inputs)
    other_inputs = other_core(layer_inputs)
    next_y = trade_y(quarters)
    next_x = trade_x(quarters)
    own = replica_params[0]
    pair = half(own, core) + other_core(half(own, 1 - core))
    key_grad = attention_keys(queries, saved_keys, saved_values, out_grad)
    own_half = lax.dynamic_slice(key_grad, (0, core * 512), (256, 512))
    other_half = other_core(lax.dynamic_slice(key_grad, (0, (1 - core) * 512), (256, 512)))
    part_a, part_b = products(layer_inputs, other_inputs, own_half, other_half)
    part_a, part_b, pair, next_y, *next_x = together(part_a, part_b, pair, next_y, *next_x)

    got_b = trade_y(part_b)
    got_a = trade_x(part_a)
    next_x = jnp.stack(next_x)
    other_x = other_core(next_x)
    other_y = other_core(next_y)
    quad = strips(pair, xh) + send(strips(pair, 1 - xh), shifted(dxh=1))
    got_b, quad, other_x, other_y, *got_a = together(got_b, quad, other_x, other_y, *got_a)

    drift = strips(half(global_params, core), xh) - quad / 4.0
    base = strips(half(global_params, core), xh) - outer_rate * (
        (1.0 + outer_beta) * drift
        + outer_beta * outer_beta * strips(half(outer_momentum, core), xh)
    )
    base_a = send(base[0], owner_a)
    base_b = send(base[1], owner_b)
    got_a = trade_y(sum_list(got_a).astype(low).reshape(4, 288, 256))
    got_b = trade_x(total(got_b).astype(low).reshape(4, 288, 256))
    base_a, base_b, got_a, *got_b = together(base_a, base_b, got_a, *got_b)

    def by_z(value):
        return jnp.stack([value[:, :128].reshape(4, 72, 128), value[:, 128:].reshape(4, 72, 128)]).reshape(8, 72, 128)

    both = jnp.stack([by_z(total(got_a).astype(low)), by_z(sum_list(got_b).astype(low))], axis=1)
    grad = total(swap(both, ("z",)))
    fresh = jnp.stack([base_a, base_b]) - (outer_rate * (1.0 + outer_beta) * step) * grad
    fresh, grad = together(fresh.astype(low), grad)

    wide = spread(fresh, ("z",), 8)
    home_a = send(grad[0], back_a)
    home_b = send(grad[1], back_b)
    wide, home_a, home_b = together(wide, home_a, home_b)

    def block(wide):
        return jnp.concatenate([wide[:4].reshape(288, 128), wide[4:].reshape(288, 128)], axis=1)

    weights_a = spread(block(wide[:, 0]), ("y",), 4).reshape(1152, 256)
    weights_b = gather_x(block(wide[:, 1])).reshape(1152, 256)
    outer = drift + step * jnp.stack([home_a, home_b])
    beside = send(outer, shifted(dxh=1))
    weights_a, weights_b, outer, beside = together(weights_a, weights_b, outer, beside)

    part_b = trade_y(project(next_y, other_y, weights_b))
    part_a = project(next_x, other_x, weights_a)
    part_a = [part_a[0], *(send(part_a[k], shifted(dx=-k)) for k in range(1, 4))]
    pair = jnp.concatenate(
        [jnp.where(xh == k, outer, beside)[ab] for ab in range(2) for k in range(2)], axis=1
    )
    across = other_core(pair)
    part_b, across, *part_a = together(part_b, across, *part_a)
    out_a = sum_list(part_a).astype(low)
    out_b = total(part_b).astype(low)
    mine = jnp.concatenate([out_a[:256], out_b[:256]], axis=1)
    theirs = other_core(jnp.concatenate([out_a[256:], out_b[256:]], axis=1))

    def by_core(own, other):
        return jnp.concatenate([jnp.where(core == k, own, other) for k in range(2)], axis=1)

    next_keys = by_core(mine, theirs)
    outer_grad = by_core(pair, across)
    fresh_momentum = outer_beta * outer_momentum + outer_grad
    fresh_params = global_params - outer_rate * (outer_grad + outer_beta * fresh_momentum)
    return (fresh_params, fresh_momentum, next_keys)


def solution(mesh):
    finer = Mesh(mesh.devices.reshape(SIZES), AXES)
    everything = REP + FSDP
    return jax.shard_map(
        body,
        mesh=finer,
        in_specs=(
            P(everything, None),
            P(everything, None),
            P(everything, None),
            P(everything, None),
            P(everything, None),
            P(FSDP, None),
            P(REP, FSDP, None),
            P(FSDP, None),
            P(everything, None),
        ),
        out_specs=(P(FSDP, None), P(FSDP, None), P(everything, None)),
        check_vma=False,
    )
```

```python
import jax
import jax.numpy as jnp
from jax import lax
from jax.experimental import pallas as pl
from jax.experimental.pallas import tpu as pltpu
from jax.sharding import Mesh
from jax.sharding import PartitionSpec as P

QH = 16
KVH = 8
HD = 128
AXES = ("xh", "core", "xl", "z", "y")
SIZES = (2, 2, 2, 8, 4)
FSDP = ("xl", "z", "y")
REP = ("xh", "core")

score_scale = 1.0 / 12.0
soft_cap = 50.0
rope_base = 10000.0
inner_rate = 0.02
outer_rate = 0.7
outer_beta = 0.9

LOW = jnp.bfloat16
WIDE = jnp.float32
ORDER = (2, 1, 3)


def place(xh, core, xl, z, y):
    return (((xh * 2 + core) * 2 + xl) * 8 + z) * 4 + y


def every_device():
    for xh in range(2):
        for core in range(2):
            for xl in range(2):
                for z in range(8):
                    for y in range(4):
                        yield xh, core, xl, z, y


def owner_route():
    route = []
    for xh, core, xl, z, y in every_device():
        zh, zl = z // 4, z % 4
        if core == 0:
            owner = place(xl, core, zh, xh * 4 + zl, y)
        else:
            owner = place(y // 2, core, y % 2, xh * 4 + zl, xl * 2 + zh)
        route.append((place(xh, core, xl, z, y), owner))
    return route


def shifted(first=0, second=0, dcore=0, dxh=0):
    route = []
    for xh, core, xl, z, y in every_device():
        dx, dy = (first, second) if core == 0 else (second, first)
        x = (xh * 2 + xl + dx + 2 * dxh) % 4
        route.append((place(xh, core, xl, z, y), place(x // 2, (core + dcore) % 2, x % 2, z, (y + dy) % 4)))
    return route


def send(value, route):
    return lax.ppermute(value, AXES, route)


def other_core(value):
    return send(value, shifted(dcore=1))


def swap_z(blocks):
    return lax.all_to_all(blocks, ("z",), 0, 0, tiled=True)


def together(*values):
    return lax.optimization_barrier(values)


def cost(flops, size, transcendentals=0):
    return pl.CostEstimate(flops=flops, bytes_accessed=size, transcendentals=transcendentals)


def like(*shape, dtype=LOW):
    return jax.ShapeDtypeStruct(shape, dtype)


def whole(*shape):
    return pl.BlockSpec(shape, lambda *_: (0,) * len(shape))


ACROSS = (((1,), (1,)), ((), ()))
DOWN = (((0,), (0,)), ((), ()))


def room(mib):
    return pltpu.CompilerParams(vmem_limit_bytes=mib << 20)


VMEM = pl.BlockSpec(memory_space=pltpu.VMEM)
SMEM = pl.BlockSpec(memory_space=pltpu.SMEM)


def attention_kernel(at_ref, query_ref, key_ref, value_ref, grad_ref, cosine_ref, sine_ref, out_ref):
    del at_ref
    rotated = None
    for g in range(QH // KVH):
        columns = slice(g * HD, (g + 1) * HD)
        for top, count in ((0, 128), (128, 256)):
            rows = slice(top, top + 128)
            query = query_ref[rows, columns]
            logits = lax.dot_general(query, key_ref[:count], ACROSS, preferred_element_type=WIDE)
            capped = jnp.tanh(logits * (score_scale / soft_cap))
            place_q = lax.broadcasted_iota(jnp.int32, (128, count), 0) + top
            place_k = lax.broadcasted_iota(jnp.int32, (128, count), 1)
            raised = jnp.where(place_q >= place_k, jnp.exp(soft_cap * capped), 0.0)
            dprobs = lax.dot_general(grad_ref[rows, columns], value_ref[:count], ACROSS, preferred_element_type=WIDE)
            inverse = 1.0 / jnp.sum(raised, axis=1, keepdims=True)
            center = jnp.sum(raised * dprobs, axis=1, keepdims=True) * inverse
            dlogits = (raised * (inverse * score_scale)) * (dprobs - center) * (1.0 - capped * capped)
            part = lax.dot_general(query, dlogits.astype(LOW), DOWN, preferred_element_type=WIDE)
            if count == 128:
                part = jnp.concatenate([part, jnp.zeros((HD, 128), WIDE)], axis=1)
            rotated = part if rotated is None else rotated + part
    first, second = rotated[: HD // 2], rotated[HD // 2 :]
    cosine, sine = cosine_ref[...], sine_ref[...]
    out_ref[: HD // 2] = (first * cosine + second * sine).astype(LOW)
    out_ref[HD // 2 :] = (second * cosine - first * sine).astype(LOW)


def attention_keys(half, cosine, sine, query_rows, key_rows, value_rows, grad_rows):
    pair = pl.BlockSpec((256, 2 * HD), lambda h, at: (0, at[0] * 4 + h))
    single = pl.BlockSpec((256, HD), lambda h, at: (0, at[0] * 4 + h))
    return pl.pallas_call(
        attention_kernel,
        grid_spec=pltpu.PrefetchScalarGridSpec(
            num_scalar_prefetch=1,
            grid=(KVH // 2,),
            in_specs=[pair, single, single, pair, whole(HD // 2, 256), whole(HD // 2, 256)],
            out_specs=pl.BlockSpec((HD, 256), lambda h, at: (h, 0)),
        ),
        out_shape=like(KVH * HD // 2, 256),
        cost_estimate=cost(500_000_000, 2_000_000, 1_000_000),
        compiler_params=room(12),
        name="attention",
    )(half, query_rows, key_rows, value_rows, grad_rows, cosine, sine)


def product_kernel(at_ref, own_ref, other_ref, grad_ref, other_grad_ref, out_ref):
    for j in range(3):
        columns = pl.ds(pl.multiple_of(at_ref[0] * 1152 + j * 384, 128), 384)
        out_ref[:, j * 384 : (j + 1) * 384] = (
            jnp.dot(grad_ref[...], own_ref[:, columns], preferred_element_type=WIDE)
            + jnp.dot(other_grad_ref[...], other_ref[:, columns], preferred_element_type=WIDE)
        ).astype(LOW)


def product(at, own, other, grad, other_grad):
    return pl.pallas_call(
        product_kernel,
        in_specs=[SMEM, VMEM, VMEM, VMEM, VMEM],
        out_specs=VMEM,
        out_shape=like(512, 1152),
        cost_estimate=cost(603_979_776, 3_000_000),
        compiler_params=room(16),
        name="product",
    )(at, own, other, grad, other_grad)


def quarter_kernel(at_ref, own_ref, other_ref, out_ref):
    del at_ref
    out_ref[:256] = own_ref[...]
    out_ref[256:] = other_ref[...]


def quarter(at, own, other):
    rows = pl.BlockSpec((256, 1152), lambda i, at: (0, at[0]))
    return pl.pallas_call(
        quarter_kernel,
        grid_spec=pltpu.PrefetchScalarGridSpec(
            num_scalar_prefetch=1, grid=(1,), in_specs=[rows, rows], out_specs=whole(512, 1152)
        ),
        out_shape=like(512, 1152),
        cost_estimate=cost(1_000_000, 2_359_296),
        compiler_params=room(16),
        name="quarter",
    )(at, own, other)


def added(refs):
    total = refs[0][...].astype(WIDE)
    for ref in refs[1:]:
        total = total + ref[...].astype(WIDE)
    return total


def first_sum_kernel(at_ref, *refs):
    ins, outs, held = refs[:4], refs[4:8], refs[8]
    held[...] = added(ins).T
    for k, out in enumerate(outs):
        place_in = (at_ref[0] + k) % 4
        for zl in range(4):
            rows = pl.ds(pl.multiple_of(zl * 288 + place_in * 72, 8), 72)
            out[zl * 72 : zl * 72 + 72] = held[rows, :].astype(LOW)


def first_sum(at, parts):
    return pl.pallas_call(
        first_sum_kernel,
        in_specs=[SMEM] + [VMEM] * 4,
        out_specs=[VMEM] * 4,
        out_shape=[like(288, 512)] * 4,
        scratch_shapes=[pltpu.VMEM((1152, 512), WIDE)],
        cost_estimate=cost(3_000_000, 6_000_000),
        compiler_params=room(24),
        name="first_sum",
    )(at, *parts)


def second_sum_kernel(*refs):
    out = refs[4]
    total = added(refs[:4])
    for high in range(2):
        for zl in range(4):
            out[high * 4 + zl] = total[zl * 72 : zl * 72 + 72, high * 256 : high * 256 + 256].astype(LOW)


def second_sum(parts):
    return pl.pallas_call(
        second_sum_kernel,
        in_specs=[VMEM] * 4,
        out_specs=VMEM,
        out_shape=like(8, 72, 256),
        cost_estimate=cost(1_000_000, 1_500_000),
        compiler_params=room(12),
        name="second_sum",
    )(*parts)


def blocks_kernel(wide_ref, out_ref):
    for high in range(2):
        for zl in range(4):
            out_ref[zl * 72 : zl * 72 + 72, high * 256 : high * 256 + 256] = wide_ref[high * 4 + zl]


def z_blocks(wide):
    return pl.pallas_call(
        blocks_kernel,
        in_specs=[VMEM],
        out_specs=VMEM,
        out_shape=like(288, 512),
        cost_estimate=cost(1_000_000, 600_000),
        compiler_params=room(8),
        name="z_blocks",
    )(wide)


def weights_kernel(at_ref, *refs):
    ins, out, held = refs[:4], refs[4], refs[5]
    for k, ref in enumerate(ins):
        place_in = (at_ref[0] + 4 - k) % 4
        for zl in range(4):
            rows = pl.ds(pl.multiple_of(zl * 288 + place_in * 72, 8), 72)
            held[rows, :] = ref[zl * 72 : zl * 72 + 72].astype(WIDE)
    out[...] = held[...].astype(LOW)


def weights(at, parts):
    return pl.pallas_call(
        weights_kernel,
        in_specs=[SMEM] + [VMEM] * 4,
        out_specs=VMEM,
        out_shape=like(1152, 512),
        scratch_shapes=[pltpu.VMEM((1152, 512), WIDE)],
        cost_estimate=cost(2_000_000, 2_500_000),
        compiler_params=room(16),
        name="weights",
    )(at, *parts)


def project_kernel(rows_ref, weights_ref, out_ref):
    out_ref[...] = jnp.dot(rows_ref[...], weights_ref[...], preferred_element_type=WIDE).astype(LOW)


def project(rows, weight):
    return pl.pallas_call(
        project_kernel,
        in_specs=[VMEM, VMEM],
        out_specs=VMEM,
        out_shape=like(512, 512),
        cost_estimate=cost(603_979_776, 3_000_000),
        compiler_params=room(16),
        name="project",
    )(rows, weight)


def last_sum_kernel(*refs):
    total = added(refs[:4])
    refs[4][...] = total[:256].astype(LOW)
    refs[5][...] = total[256:].astype(LOW)


def last_sum(parts):
    return pl.pallas_call(
        last_sum_kernel,
        in_specs=[VMEM] * 4,
        out_specs=[VMEM] * 2,
        out_shape=[like(256, 512)] * 2,
        cost_estimate=cost(1_000_000, 2_500_000),
        compiler_params=room(12),
        name="last_sum",
    )(*parts)


def body(
    layer_inputs,
    queries,
    saved_keys,
    saved_values,
    out_grad,
    global_params,
    replica_params,
    outer_momentum,
    next_inputs,
):
    to_owner = owner_route()
    to_home = [(j, i) for i, j in to_owner]
    core = lax.axis_index("core")
    xh = lax.axis_index("xh")
    x = xh * 2 + lax.axis_index("xl")
    y = lax.axis_index("y")
    first = jnp.where(core == 0, x, y)
    second = jnp.where(core == 0, y, x)
    step = inner_rate / 4.0

    def scalar(value):
        return value.astype(jnp.int32).reshape(1)

    def strip(value, c, h):
        return lax.dynamic_slice(value, (0, c * 512 + h * 256), (72, 256))

    freqs = rope_base ** (-jnp.arange(HD // 2).astype(WIDE) / (HD // 2))
    angles = freqs[:, None] * jnp.arange(256).astype(WIDE)[None, :]
    other_inputs = other_core(layer_inputs)
    other_next = other_core(next_inputs)
    saved = (jnp.cos(angles), jnp.sin(angles), queries, saved_keys, saved_values, out_grad)
    other_half = other_core(attention_keys(scalar(1 - core), *saved))
    own_half = attention_keys(scalar(core), *saved)

    got = {}
    for k in (*ORDER, 0):
        part = product(scalar((first + k) % 4), layer_inputs, other_inputs, own_half, other_half)
        got[k] = send(part, shifted(first=k)) if k else part
    got[0], own, next_inputs, other_next = together(got[0], replica_params[0], next_inputs, other_next)
    rep_sum = strip(own, core, xh)
    for dc, dh in ((1, 0), (0, 1), (1, 1)):
        there = strip(own, (core + dc) % 2, (xh + dh) % 2)
        rep_sum = rep_sum + send(there, shifted(dcore=dc, dxh=dh))
    cut = [quarter(scalar((first + k) % 4), next_inputs, other_next) for k in range(4)]
    got, rep_sum, cut = together(got, rep_sum, cut)

    sums = first_sum(scalar(second), [got[k] for k in range(4)])
    got = {0: sums[0]}
    for k in ORDER:
        got[k] = send(sums[k], shifted(second=k))
    drift = strip(global_params, core, xh) - rep_sum / 4.0
    base = strip(global_params, core, xh) - outer_rate * (
        (1.0 + outer_beta) * drift + outer_beta * outer_beta * strip(outer_momentum, core, xh)
    )
    base = send(base, to_owner)
    got, cut, base, drift = together(got, cut, base, drift)

    moved = [cut[0], *(send(cut[k], shifted(first=k)) for k in range(1, 4))]
    grad = jnp.sum(swap_z(second_sum([got[k] for k in range(4)])).astype(WIDE), axis=0)
    fresh = base - (outer_rate * (1.0 + outer_beta) * step) * grad
    fresh, grad = together(fresh.astype(LOW), grad)

    block = z_blocks(swap_z(jnp.broadcast_to(fresh[None], (8, 72, 256))))
    block, moved, grad = together(block, moved, grad)

    parts = {0: block}
    for k in ORDER:
        parts[k] = send(block, shifted(second=k))
    home = send(grad, to_home)
    parts, home = together(parts, home)

    weight = weights(scalar(second), [parts[k] for k in range(4)])
    out = {}
    for k in (*ORDER, 0):
        part = project(moved[k], weight)
        out[k] = send(part, shifted(first=-k)) if k else part
    outer = drift + step * home
    beside = send(outer, shifted(dxh=1))
    out, outer, beside = together(out, outer, beside)

    mine, theirs = last_sum([out[k] for k in range(4)])
    theirs = other_core(theirs)
    pair = jnp.concatenate([jnp.where(xh == h, outer, beside) for h in range(2)], axis=1)
    across = other_core(pair)

    def by_core(own, other):
        return jnp.concatenate([jnp.where(core == c, own, other) for c in range(2)], axis=1)

    next_keys = by_core(mine, theirs)
    outer_grad = by_core(pair, across)
    fresh_momentum = outer_beta * outer_momentum + outer_grad
    fresh_params = global_params - outer_rate * (outer_grad + outer_beta * fresh_momentum)
    return (fresh_params, fresh_momentum, next_keys)


def solution(mesh):
    finer = Mesh(mesh.devices.reshape(SIZES), AXES)
    everything = REP + FSDP
    return jax.shard_map(
        body,
        mesh=finer,
        in_specs=(
            P(everything, None),
            P(everything, None),
            P(everything, None),
            P(everything, None),
            P(everything, None),
            P(FSDP, None),
            P(REP, FSDP, None),
            P(FSDP, None),
            P(everything, None),
        ),
        out_specs=(P(FSDP, None), P(FSDP, None), P(everything, None)),
        check_vma=False,
    )
```

```python
import jax
import jax.numpy as jnp
from jax import lax
from jax.experimental import pallas as pl
from jax.experimental.pallas import tpu as pltpu
from jax.sharding import Mesh
from jax.sharding import PartitionSpec as P

KVH = 8
HD = 128
AXES = ("xh", "core", "xl", "z", "y")
SIZES = (2, 2, 2, 8, 4)
FSDP = ("xl", "z", "y")
REP = ("xh", "core")

score_scale = 1.0 / 12.0
soft_cap = 50.0
rope_base = 10000.0
inner_rate = 0.02
outer_rate = 0.7
outer_beta = 0.9

LOW = jnp.bfloat16
WIDE = jnp.float32
ORDER = (2, 1, 3)


def place(xh, core, xl, z, y):
    return (((xh * 2 + core) * 2 + xl) * 8 + z) * 4 + y


def every_device():
    for xh in range(2):
        for core in range(2):
            for xl in range(2):
                for z in range(8):
                    for y in range(4):
                        yield xh, core, xl, z, y


def owner_route(dcore=0, dxh=0):
    route = []
    for xh, core, xl, z, y in every_device():
        zh, zl = z // 4, z % 4
        home = place((xh + dxh) % 2, (core + dcore) % 2, xl, z, y)
        if core == 0:
            owner = place(xl, core, zh, xh * 4 + zl, y)
        else:
            owner = place(y // 2, core, y % 2, xh * 4 + zl, xl * 2 + zh)
        route.append((home, owner))
    return route


def shifted(first=0, second=0, dcore=0, dxh=0):
    route = []
    for xh, core, xl, z, y in every_device():
        dx, dy = (first, second) if core == 0 else (second, first)
        x = (xh * 2 + xl + dx + 2 * dxh) % 4
        route.append((place(xh, core, xl, z, y), place(x // 2, (core + dcore) % 2, x % 2, z, (y + dy) % 4)))
    return route


def send(value, route):
    return lax.ppermute(value, AXES, route)


def other_core(value):
    return send(value, shifted(dcore=1))


def swap_z(blocks):
    return lax.all_to_all(blocks, ("z",), 0, 0, tiled=True)


def together(*values):
    return lax.optimization_barrier(values)


def cost(flops, size, transcendentals=0):
    return pl.CostEstimate(flops=flops, bytes_accessed=size, transcendentals=transcendentals)


def like(*shape, dtype=LOW):
    return jax.ShapeDtypeStruct(shape, dtype)


def whole(*shape):
    return pl.BlockSpec(shape, lambda *_: (0,) * len(shape))


ACROSS = (((1,), (1,)), ((), ()))
DOWN = (((0,), (0,)), ((), ()))


def room(mib):
    return pltpu.CompilerParams(vmem_limit_bytes=mib << 20)


VMEM = pl.BlockSpec(memory_space=pltpu.VMEM)
SMEM = pl.BlockSpec(memory_space=pltpu.SMEM)


def attention_kernel(at_ref, query_ref, key_ref, value_ref, grad_ref, cosine_ref, sine_ref, out_ref):
    del at_ref
    cosine, sine = cosine_ref[...], sine_ref[...]
    seen = lax.broadcasted_iota(jnp.int32, (256, 256), 0) >= lax.broadcasted_iota(jnp.int32, (256, 256), 1)
    for h in range(2):
        key, value = key_ref[:, h * HD : (h + 1) * HD], value_ref[:, h * HD : (h + 1) * HD]
        rotated = jnp.zeros((HD, 256), WIDE)
        for j in (2 * h, 2 * h + 1):
            query, grad = query_ref[:, j * HD : (j + 1) * HD], grad_ref[:, j * HD : (j + 1) * HD]
            logits = lax.dot_general(query, key, ACROSS, preferred_element_type=WIDE)
            capped = jnp.tanh(logits * (score_scale / soft_cap))
            raised = jnp.where(seen, jnp.exp(soft_cap * capped), 0.0)
            dprobs = lax.dot_general(grad, value, ACROSS, preferred_element_type=WIDE)
            inverse = 1.0 / jnp.sum(raised, axis=1, keepdims=True)
            center = jnp.sum(raised * dprobs, axis=1, keepdims=True) * inverse
            dlogits = (raised * (inverse * score_scale)) * (dprobs - center) * (1.0 - capped * capped)
            rotated = rotated + lax.dot_general(query, dlogits.astype(LOW), DOWN, preferred_element_type=WIDE)
        first, second = rotated[: HD // 2], rotated[HD // 2 :]
        out_ref[h * HD : h * HD + HD // 2] = (first * cosine + second * sine).astype(LOW)
        out_ref[h * HD + HD // 2 : (h + 1) * HD] = (second * cosine - first * sine).astype(LOW)


def attention_keys(half, cosine, sine, query_rows, key_rows, value_rows, grad_rows):
    pair = pl.BlockSpec((256, 4 * HD), lambda h, at: (0, at[0] * 2 + h))
    single = pl.BlockSpec((256, 2 * HD), lambda h, at: (0, at[0] * 2 + h))
    return pl.pallas_call(
        attention_kernel,
        grid_spec=pltpu.PrefetchScalarGridSpec(
            num_scalar_prefetch=1,
            grid=(KVH // 4,),
            in_specs=[pair, single, single, pair, whole(HD // 2, 256), whole(HD // 2, 256)],
            out_specs=pl.BlockSpec((2 * HD, 256), lambda h, at: (h, 0)),
        ),
        out_shape=like(KVH * HD // 2, 256),
        cost_estimate=cost(500_000_000, 2_000_000, 1_000_000),
        name="attention",
    )(half, query_rows, key_rows, value_rows, grad_rows, cosine, sine)


def product_kernel(at_ref, own_ref, other_ref, grad_ref, other_grad_ref, out_ref):
    for j in range(3):
        columns = pl.ds(pl.multiple_of(at_ref[0] * 1152 + j * 384, 128), 384)
        out_ref[:, j * 384 : (j + 1) * 384] = (
            jnp.dot(grad_ref[...], own_ref[:, columns], preferred_element_type=WIDE)
            + jnp.dot(other_grad_ref[...], other_ref[:, columns], preferred_element_type=WIDE)
        ).astype(LOW)


def product(at, own, other, grad, other_grad):
    return pl.pallas_call(
        product_kernel,
        in_specs=[SMEM, VMEM, VMEM, VMEM, VMEM],
        out_specs=VMEM,
        out_shape=like(512, 1152),
        cost_estimate=cost(603_979_776, 3_000_000),
        compiler_params=room(16),
        name="product",
    )(at, own, other, grad, other_grad)


def quarter_kernel(at_ref, own_ref, other_ref, out_ref):
    del at_ref
    out_ref[:256] = own_ref[...]
    out_ref[256:] = other_ref[...]


def quarter(at, own, other):
    rows = pl.BlockSpec((256, 1152), lambda i, at: (0, at[0]))
    return pl.pallas_call(
        quarter_kernel,
        grid_spec=pltpu.PrefetchScalarGridSpec(
            num_scalar_prefetch=1, grid=(1,), in_specs=[rows, rows], out_specs=whole(512, 1152)
        ),
        out_shape=like(512, 1152),
        cost_estimate=cost(1_000_000, 2_359_296),
        compiler_params=room(16),
        name="quarter",
    )(at, own, other)


def added(refs):
    total = refs[0][...].astype(WIDE)
    for ref in refs[1:]:
        total = total + ref[...].astype(WIDE)
    return total


def first_sum_kernel(at_ref, *refs):
    ins, outs, held = refs[:4], refs[4:8], refs[8]
    held[...] = added(ins).T
    for k, out in enumerate(outs):
        place_in = (at_ref[0] + k) % 4
        for zl in range(4):
            rows = pl.ds(pl.multiple_of(zl * 288 + place_in * 72, 8), 72)
            out[zl * 72 : zl * 72 + 72] = held[rows, :].astype(LOW)


def first_sum(at, parts):
    return pl.pallas_call(
        first_sum_kernel,
        in_specs=[SMEM] + [VMEM] * 4,
        out_specs=[VMEM] * 4,
        out_shape=[like(288, 512)] * 4,
        scratch_shapes=[pltpu.VMEM((1152, 512), WIDE)],
        cost_estimate=cost(3_000_000, 6_000_000),
        compiler_params=room(24),
        name="first_sum",
    )(at, *parts)


def second_sum_kernel(*refs):
    out = refs[4]
    total = added(refs[:4])
    for high in range(2):
        for zl in range(4):
            out[high * 4 + zl] = total[zl * 72 : zl * 72 + 72, high * 256 : high * 256 + 256].astype(LOW)


def second_sum(parts):
    return pl.pallas_call(
        second_sum_kernel,
        in_specs=[VMEM] * 4,
        out_specs=VMEM,
        out_shape=like(8, 72, 256),
        cost_estimate=cost(1_000_000, 1_500_000),
        compiler_params=room(12),
        name="second_sum",
    )(*parts)


def blocks_kernel(wide_ref, out_ref):
    for high in range(2):
        for zl in range(4):
            out_ref[zl * 72 : zl * 72 + 72, high * 256 : high * 256 + 256] = wide_ref[high * 4 + zl]


def z_blocks(wide):
    return pl.pallas_call(
        blocks_kernel,
        in_specs=[VMEM],
        out_specs=VMEM,
        out_shape=like(288, 512),
        cost_estimate=cost(1_000_000, 600_000),
        compiler_params=room(8),
        name="z_blocks",
    )(wide)


def weights_kernel(at_ref, *refs):
    ins, out, held = refs[:4], refs[4], refs[5]
    for k, ref in enumerate(ins):
        place_in = (at_ref[0] + 4 - k) % 4
        for zl in range(4):
            rows = pl.ds(pl.multiple_of(zl * 288 + place_in * 72, 8), 72)
            held[rows, :] = ref[zl * 72 : zl * 72 + 72].astype(WIDE)
    out[...] = held[...].astype(LOW)


def weights(at, parts):
    return pl.pallas_call(
        weights_kernel,
        in_specs=[SMEM] + [VMEM] * 4,
        out_specs=VMEM,
        out_shape=like(1152, 512),
        scratch_shapes=[pltpu.VMEM((1152, 512), WIDE)],
        cost_estimate=cost(2_000_000, 2_500_000),
        compiler_params=room(16),
        name="weights",
    )(at, *parts)


def project_kernel(rows_ref, weights_ref, out_ref):
    out_ref[...] = jnp.dot(rows_ref[...], weights_ref[...], preferred_element_type=WIDE).astype(LOW)


def project(rows, weight):
    return pl.pallas_call(
        project_kernel,
        in_specs=[VMEM, VMEM],
        out_specs=VMEM,
        out_shape=like(512, 512),
        cost_estimate=cost(603_979_776, 3_000_000),
        compiler_params=room(16),
        name="project",
    )(rows, weight)


def last_sum_kernel(*refs):
    total = added(refs[:4])
    refs[4][...] = total[:256].astype(LOW)
    refs[5][...] = total[256:].astype(LOW)


def last_sum(parts):
    return pl.pallas_call(
        last_sum_kernel,
        in_specs=[VMEM] * 4,
        out_specs=[VMEM] * 2,
        out_shape=[like(256, 512)] * 2,
        cost_estimate=cost(1_000_000, 2_500_000),
        compiler_params=room(12),
        name="last_sum",
    )(*parts)


def body(
    layer_inputs,
    queries,
    saved_keys,
    saved_values,
    out_grad,
    global_params,
    replica_params,
    outer_momentum,
    next_inputs,
):
    to_home = [(j, i) for i, j in owner_route()]
    core = lax.axis_index("core")
    xh = lax.axis_index("xh")
    x = xh * 2 + lax.axis_index("xl")
    y = lax.axis_index("y")
    first = jnp.where(core == 0, x, y)
    second = jnp.where(core == 0, y, x)
    step = inner_rate / 4.0

    def sum_of(values):
        return values[0] + values[1] + values[2] + values[3]

    def scalar(value):
        return value.astype(jnp.int32).reshape(1)

    def strip(value, c, h):
        return lax.dynamic_slice(value, (0, c * 512 + h * 256), (72, 256))

    freqs = rope_base ** (-jnp.arange(HD // 2).astype(WIDE) / (HD // 2))
    angles = freqs[:, None] * jnp.arange(256).astype(WIDE)[None, :]
    other_inputs = other_core(layer_inputs)
    saved = (jnp.cos(angles), jnp.sin(angles), queries, saved_keys, saved_values, out_grad)
    other_half, other_inputs = together(attention_keys(scalar(1 - core), *saved), other_inputs)
    other_half = other_core(other_half)
    own_half = attention_keys(scalar(core), *saved)

    got = {}
    for k in (*ORDER, 0):
        part = product(scalar((first + k) % 4), layer_inputs, other_inputs, own_half, other_half)
        got[k] = send(part, shifted(first=k)) if k else part
    other_next = other_core(next_inputs)
    own = replica_params[0]
    rep_parts = [strip(own, core, xh)]
    for dc, dh in ((1, 0), (0, 1), (1, 1)):
        there = strip(own, (core + dc) % 2, (xh + dh) % 2)
        rep_parts.append(send(there, shifted(dcore=dc, dxh=dh)))
    cut = [quarter(scalar((first + k) % 4), next_inputs, other_next) for k in range(1, 4)]
    got, cut, rep_parts, other_next = together(got, cut, rep_parts, other_next)

    sums = first_sum(scalar(second), [got[k] for k in range(4)])
    got = {0: sums[0]}
    for k in ORDER:
        got[k] = send(sums[k], shifted(second=k))
    drift = strip(global_params, core, xh) - sum_of(rep_parts) / 4.0
    still = strip(global_params, core, xh) - (outer_rate * outer_beta * outer_beta) * strip(outer_momentum, core, xh)
    base = still - (outer_rate * (1.0 + outer_beta)) * drift
    base = send(base, owner_route())
    got, cut, drift, other_next = together(got, cut, drift, other_next)

    blocks = second_sum([got[k] for k in range(4)])
    blocks = swap_z(blocks)
    moved = {k: send(cut[k - 1], shifted(first=k)) for k in ORDER}
    moved[0] = quarter(scalar(first), next_inputs, other_next)
    grad = jnp.sum(blocks.astype(WIDE), axis=0)
    fresh = base - (outer_rate * (1.0 + outer_beta) * step) * grad
    fresh, grad = together(fresh.astype(LOW), grad)

    wide = swap_z(jnp.broadcast_to(fresh[None], (8, 72, 256)))
    block = z_blocks(wide)
    block, grad = together(block, grad)

    parts = {0: block}
    for k in ORDER:
        parts[k] = send(block, shifted(second=k))
    parts, grad = together(parts, grad)

    weight = weights(scalar(second), [parts[k] for k in range(4)])
    out = {}
    for k in (*ORDER, 0):
        part = project(moved[k], weight)
        out[k] = send(part, shifted(first=-k)) if k else part
    outer = drift + step * send(grad, to_home)
    beside = send(outer, shifted(dxh=1))
    pair = jnp.concatenate([jnp.where(xh == h, outer, beside) for h in range(2)], axis=1)
    across = other_core(pair)
    (out,) = together(out)

    mine, theirs = last_sum([out[k] for k in range(4)])
    theirs = other_core(theirs)

    def by_core(own, other):
        return jnp.concatenate([jnp.where(core == c, own, other) for c in range(2)], axis=1)

    next_keys = by_core(mine, theirs)
    outer_grad = by_core(pair, across)
    fresh_momentum = outer_beta * outer_momentum + outer_grad
    fresh_params = global_params - outer_rate * (outer_grad + outer_beta * fresh_momentum)
    return (fresh_params, fresh_momentum, next_keys)


def solution(mesh):
    finer = Mesh(mesh.devices.reshape(SIZES), AXES)
    everything = REP + FSDP
    return jax.shard_map(
        body,
        mesh=finer,
        in_specs=(
            P(everything, None),
            P(everything, None),
            P(everything, None),
            P(everything, None),
            P(everything, None),
            P(FSDP, None),
            P(REP, FSDP, None),
            P(FSDP, None),
            P(everything, None),
        ),
        out_specs=(P(FSDP, None), P(FSDP, None), P(everything, None)),
        check_vma=False,
    )
```

```python
import jax
import jax.numpy as jnp
import numpy as np
from jax import lax
from jax.experimental import pallas as pl
from jax.experimental.pallas import tpu as pltpu
from jax.sharding import Mesh
from jax.sharding import PartitionSpec as P

KVH = 8
HD = 128
AXES = ("xh", "core", "xl", "z", "y")
SIZES = (2, 2, 2, 8, 4)
FSDP = ("xl", "z", "y")
REP = ("xh", "core")

score_scale = 1.0 / 12.0
soft_cap = 50.0
rope_base = 10000.0
inner_rate = 0.02
outer_rate = 0.7
outer_beta = 0.9

LOW = jnp.bfloat16
WIDE = jnp.float32
ORDER = (2, 1, 3)


def place(xh, core, xl, z, y):
    return (((xh * 2 + core) * 2 + xl) * 8 + z) * 4 + y


def every_device():
    for xh in range(2):
        for core in range(2):
            for xl in range(2):
                for z in range(8):
                    for y in range(4):
                        yield xh, core, xl, z, y


def along_z(high, low):
    return (low + 2 + 4 * high) % 8


def owner_route(dcore=0, dxh=0):
    route = []
    for xh, core, xl, z, y in every_device():
        zh, zl = z // 4, z % 4
        home = place((xh + dxh) % 2, (core + dcore) % 2, xl, z, y)
        if core == 0:
            owner = place(xl, core, zh, along_z(xh, zl), y)
        else:
            owner = place(y // 2, core, y % 2, along_z(xh, zl), xl * 2 + zh)
        route.append((home, owner))
    return route


def shifted(first=0, second=0, dcore=0, dxh=0):
    route = []
    for xh, core, xl, z, y in every_device():
        dx, dy = (first, second) if core == 0 else (second, first)
        x = (xh * 2 + xl + dx + 2 * dxh) % 4
        route.append((place(xh, core, xl, z, y), place(x // 2, (core + dcore) % 2, x % 2, z, (y + dy) % 4)))
    return route


def send(value, route):
    return lax.ppermute(value, AXES, route)


def other_core(value):
    return send(value, shifted(dcore=1))


def swap_z(blocks):
    return lax.all_to_all(blocks, ("z",), 0, 0, tiled=True)


def together(*values):
    return lax.optimization_barrier(values)


def cost(flops, size, transcendentals=0):
    return pl.CostEstimate(flops=flops, bytes_accessed=size, transcendentals=transcendentals)


def like(*shape, dtype=LOW):
    return jax.ShapeDtypeStruct(shape, dtype)


def whole(*shape):
    return pl.BlockSpec(shape, lambda *_: (0,) * len(shape))


ACROSS = (((1,), (1,)), ((), ()))
DOWN = (((0,), (0,)), ((), ()))


def room(mib):
    return pltpu.CompilerParams(vmem_limit_bytes=mib << 20)


VMEM = pl.BlockSpec(memory_space=pltpu.VMEM)
SMEM = pl.BlockSpec(memory_space=pltpu.SMEM)


def attention_kernel(at_ref, query_ref, key_ref, value_ref, grad_ref, cosine_ref, sine_ref, out_ref):
    del at_ref
    cosine, sine = cosine_ref[...], sine_ref[...]
    seen = lax.broadcasted_iota(jnp.int32, (256, 256), 0) >= lax.broadcasted_iota(jnp.int32, (256, 256), 1)
    for h in range(2):
        key, value = key_ref[:, h * HD : (h + 1) * HD], value_ref[:, h * HD : (h + 1) * HD]
        rotated = jnp.zeros((HD, 256), WIDE)
        for j in (2 * h, 2 * h + 1):
            query, grad = query_ref[:, j * HD : (j + 1) * HD], grad_ref[:, j * HD : (j + 1) * HD]
            logits = lax.dot_general(query, key, ACROSS, preferred_element_type=WIDE)
            capped = jnp.tanh(logits * (score_scale / soft_cap))
            raised = jnp.where(seen, jnp.exp(soft_cap * capped), 0.0)
            dprobs = lax.dot_general(grad, value, ACROSS, preferred_element_type=WIDE)
            inverse = 1.0 / jnp.sum(raised, axis=1, keepdims=True)
            center = jnp.sum(raised * dprobs, axis=1, keepdims=True) * inverse
            dlogits = (raised * (inverse * score_scale)) * (dprobs - center) * (1.0 - capped * capped)
            rotated = rotated + lax.dot_general(query, dlogits.astype(LOW), DOWN, preferred_element_type=WIDE)
        first, second = rotated[: HD // 2], rotated[HD // 2 :]
        out_ref[h * HD : h * HD + HD // 2] = (first * cosine + second * sine).astype(LOW)
        out_ref[h * HD + HD // 2 : (h + 1) * HD] = (second * cosine - first * sine).astype(LOW)


def attention_keys(half, cosine, sine, query_rows, key_rows, value_rows, grad_rows):
    pair = pl.BlockSpec((256, 4 * HD), lambda h, at: (0, at[0] * 2 + h))
    single = pl.BlockSpec((256, 2 * HD), lambda h, at: (0, at[0] * 2 + h))
    return pl.pallas_call(
        attention_kernel,
        grid_spec=pltpu.PrefetchScalarGridSpec(
            num_scalar_prefetch=1,
            grid=(KVH // 4,),
            in_specs=[pair, single, single, pair, whole(HD // 2, 256), whole(HD // 2, 256)],
            out_specs=pl.BlockSpec((2 * HD, 256), lambda h, at: (h, 0)),
        ),
        out_shape=like(KVH * HD // 2, 256),
        cost_estimate=cost(500_000_000, 2_000_000, 1_000_000),
        name="attention",
    )(half, query_rows, key_rows, value_rows, grad_rows, cosine, sine)


def product_kernel(at_ref, own_ref, other_ref, grad_ref, other_grad_ref, out_ref):
    del at_ref
    out_ref[...] = (
        jnp.dot(grad_ref[...], own_ref[...], preferred_element_type=WIDE)
        + jnp.dot(other_grad_ref[...], other_ref[...], preferred_element_type=WIDE)
    ).astype(LOW)


def product(at, own, other, grad, other_grad):
    rows = pl.BlockSpec((256, 1152), lambda i, at: (0, at[0]))
    return pl.pallas_call(
        product_kernel,
        grid_spec=pltpu.PrefetchScalarGridSpec(
            num_scalar_prefetch=1,
            grid=(1,),
            in_specs=[rows, rows, VMEM, VMEM],
            out_specs=whole(512, 1152),
        ),
        out_shape=like(512, 1152),
        cost_estimate=cost(603_979_776, 3_000_000),
        name="product",
    )(at, own, other, grad, other_grad)


def quarter_kernel(at_ref, own_ref, other_ref, out_ref):
    del at_ref
    out_ref[:256] = own_ref[...]
    out_ref[256:] = other_ref[...]


def quarter(at, own, other):
    rows = pl.BlockSpec((256, 1152), lambda i, at: (0, at[0]))
    return pl.pallas_call(
        quarter_kernel,
        grid_spec=pltpu.PrefetchScalarGridSpec(
            num_scalar_prefetch=1, grid=(1,), in_specs=[rows, rows], out_specs=whole(512, 1152)
        ),
        out_shape=like(512, 1152),
        cost_estimate=cost(1_000_000, 2_359_296),
        compiler_params=room(16),
        name="quarter",
    )(at, own, other)


def added(refs):
    total = refs[0][...].astype(WIDE)
    for ref in refs[1:]:
        total = total + ref[...].astype(WIDE)
    return total


def first_sum_kernel(at_ref, *refs):
    ins, outs, held = refs[:4], refs[4:8], refs[8]
    held[...] = added(ins).T
    for k, out in enumerate(outs):
        place_in = (at_ref[0] + k) % 4
        for zl in range(4):
            rows = pl.ds(pl.multiple_of(zl * 288 + place_in * 72, 8), 72)
            out[zl * 72 : zl * 72 + 72] = held[rows, :].astype(LOW)


def first_sum(at, parts):
    return pl.pallas_call(
        first_sum_kernel,
        in_specs=[SMEM] + [VMEM] * 4,
        out_specs=[VMEM] * 4,
        out_shape=[like(288, 512)] * 4,
        scratch_shapes=[pltpu.VMEM((1152, 512), WIDE)],
        cost_estimate=cost(3_000_000, 6_000_000),
        compiler_params=room(24),
        name="first_sum",
    )(at, *parts)


def second_sum_kernel(*refs):
    out = refs[4]
    total = added(refs[:4])
    for high in range(2):
        for zl in range(4):
            out[along_z(high, zl)] = total[zl * 72 : zl * 72 + 72, high * 256 : high * 256 + 256].astype(LOW)


def second_sum(parts):
    return pl.pallas_call(
        second_sum_kernel,
        in_specs=[VMEM] * 4,
        out_specs=VMEM,
        out_shape=like(8, 72, 256),
        cost_estimate=cost(1_000_000, 1_500_000),
        compiler_params=room(12),
        name="second_sum",
    )(*parts)


def update_kernel(blocks_ref, base_ref, wide_ref, outer_ref):
    grad = blocks_ref[0].astype(WIDE)
    for k in range(1, 8):
        grad = grad + blocks_ref[k].astype(WIDE)
    outer = base_ref[1] + (inner_rate / 4.0) * grad
    outer_ref[...] = outer
    fresh = (base_ref[0] - (outer_rate * (1.0 + outer_beta)) * outer).astype(LOW)
    for k in range(8):
        wide_ref[k] = fresh


def update(blocks, base):
    return pl.pallas_call(
        update_kernel,
        in_specs=[VMEM] * 2,
        out_specs=[VMEM] * 2,
        out_shape=[like(8, 72, 256), like(72, 256, dtype=WIDE)],
        cost_estimate=cost(1_000_000, 700_000),
        compiler_params=room(8),
        name="update",
    )(blocks, base)


def blocks_kernel(wide_ref, out_ref):
    for high in range(2):
        for zl in range(4):
            out_ref[zl * 72 : zl * 72 + 72, high * 256 : high * 256 + 256] = wide_ref[along_z(high, zl)]


def z_blocks(wide):
    return pl.pallas_call(
        blocks_kernel,
        in_specs=[VMEM],
        out_specs=VMEM,
        out_shape=like(288, 512),
        cost_estimate=cost(1_000_000, 600_000),
        compiler_params=room(8),
        name="z_blocks",
    )(wide)


def weights_kernel(at_ref, *refs):
    ins, out, held = refs[:4], refs[4], refs[5]
    for k, ref in enumerate(ins):
        place_in = (at_ref[0] + 4 - k) % 4
        for zl in range(4):
            rows = pl.ds(pl.multiple_of(zl * 288 + place_in * 72, 8), 72)
            held[rows, :] = ref[zl * 72 : zl * 72 + 72].astype(WIDE)
    out[...] = held[...].astype(LOW)


def weights(at, parts):
    return pl.pallas_call(
        weights_kernel,
        in_specs=[SMEM] + [VMEM] * 4,
        out_specs=VMEM,
        out_shape=like(1152, 512),
        scratch_shapes=[pltpu.VMEM((1152, 512), WIDE)],
        cost_estimate=cost(2_000_000, 2_500_000),
        compiler_params=room(16),
        name="weights",
    )(at, *parts)


def project_kernel(rows_ref, weights_ref, out_ref):
    out_ref[...] = jnp.dot(rows_ref[...], weights_ref[...], preferred_element_type=WIDE).astype(LOW)


def project(rows, weight):
    return pl.pallas_call(
        project_kernel,
        in_specs=[VMEM, VMEM],
        out_specs=VMEM,
        out_shape=like(512, 512),
        cost_estimate=cost(603_979_776, 3_000_000),
        compiler_params=room(16),
        name="project",
    )(rows, weight)


def last_sum_kernel(*refs):
    total = added(refs[:4])
    refs[4][...] = total[:256].astype(LOW)
    refs[5][...] = total[256:].astype(LOW)


def last_sum(parts):
    return pl.pallas_call(
        last_sum_kernel,
        in_specs=[VMEM] * 4,
        out_specs=[VMEM] * 2,
        out_shape=[like(256, 512)] * 2,
        cost_estimate=cost(1_000_000, 2_500_000),
        compiler_params=room(12),
        name="last_sum",
    )(*parts)


def join_kernel(at_ref, mine_ref, theirs_ref, out_ref):
    core = at_ref[0]
    out_ref[:, pl.ds(pl.multiple_of(core * 512, 128), 512)] = mine_ref[...]
    out_ref[:, pl.ds(pl.multiple_of((1 - core) * 512, 128), 512)] = theirs_ref[...]


def join(at, mine, theirs):
    return pl.pallas_call(
        join_kernel,
        in_specs=[SMEM, VMEM, VMEM],
        out_specs=VMEM,
        out_shape=like(256, 1024),
        cost_estimate=cost(1_000_000, 1_000_000),
        compiler_params=room(8),
        name="join",
    )(at, mine, theirs)


def body(
    layer_inputs,
    queries,
    saved_keys,
    saved_values,
    out_grad,
    global_params,
    replica_params,
    outer_momentum,
    next_inputs,
):
    to_home = [(j, i) for i, j in owner_route()]
    other_home = dict(shifted(dxh=1))
    to_other_home = [(j, other_home[i]) for j, i in to_home]
    core = lax.axis_index("core")
    xh = lax.axis_index("xh")
    x = xh * 2 + lax.axis_index("xl")
    y = lax.axis_index("y")
    first = jnp.where(core == 0, x, y)
    second = jnp.where(core == 0, y, x)

    def sum_of(values):
        return values[0] + values[1] + values[2] + values[3]

    def scalar(value):
        return value.astype(jnp.int32).reshape(1)

    def strip(value, c, h):
        return lax.dynamic_slice(value, (0, c * 512 + h * 256), (72, 256))

    freqs = np.float32(rope_base) ** (-np.arange(HD // 2, dtype=np.float32) / np.float32(HD // 2))
    angles = (freqs[:, None] * np.arange(256, dtype=np.float32)[None, :]).astype(np.float32)
    other_inputs = other_core(layer_inputs)
    saved = (np.cos(angles), np.sin(angles), queries, saved_keys, saved_values, out_grad)
    other_half, other_inputs = together(attention_keys(scalar(1 - core), *saved), other_inputs)
    other_half = other_core(other_half)
    own_half = attention_keys(scalar(core), *saved)

    got = {}
    for k in (*ORDER, 0):
        part = product(scalar((first + k) % 4), layer_inputs, other_inputs, own_half, other_half)
        got[k] = send(part, shifted(first=k)) if k else part
    other_next = other_core(next_inputs)
    own = replica_params[0]
    rep_parts = [strip(own, core, xh)]
    for dc, dh in ((1, 0), (0, 1), (1, 1)):
        there = strip(own, (core + dc) % 2, (xh + dh) % 2)
        rep_parts.append(send(there, shifted(dcore=dc, dxh=dh)))
    cut = [quarter(scalar((first + k) % 4), next_inputs, other_next) for k in range(1, 4)]
    got, cut, other_next = together(got, cut, other_next)

    sums = first_sum(scalar(second), [got[k] for k in range(4)])
    got = {0: sums[0]}
    for k in ORDER:
        got[k] = send(sums[k], shifted(second=k))
    drift = strip(global_params, core, xh) - sum_of(rep_parts) / 4.0
    still = strip(global_params, core, xh) - (outer_rate * outer_beta * outer_beta) * strip(outer_momentum, core, xh)
    base = send(jnp.stack([still, drift]), owner_route())
    got, cut, other_next = together(got, cut, other_next)

    blocks = second_sum([got[k] for k in range(4)])
    blocks = swap_z(blocks)
    moved = {k: send(cut[k - 1], shifted(first=k)) for k in ORDER}
    moved[0] = quarter(scalar(first), next_inputs, other_next)
    wide, outer = update(blocks, base)
    wide, outer = together(wide, outer)
    near = send(outer, to_home)
    far = send(outer, to_other_home)

    wide = swap_z(wide)
    block = z_blocks(wide)
    (block,) = together(block)

    parts = {0: block}
    for k in ORDER:
        parts[k] = send(block, shifted(second=k))
    (parts,) = together(parts)

    weight = weights(scalar(second), [parts[k] for k in range(4)])
    out = {}
    for k in ORDER:
        part = project(moved[k], weight)
        out[k] = send(part, shifted(first=-k))
    out[0] = project(moved[0], weight)
    pair = jnp.concatenate([jnp.where(xh == h, near, far) for h in range(2)], axis=1)
    across = other_core(pair)
    (out,) = together(out)

    mine, theirs = last_sum([out[k] for k in range(4)])
    theirs = other_core(theirs)

    def by_core(own, other):
        return jnp.concatenate([jnp.where(core == c, own, other) for c in range(2)], axis=1)

    next_keys = join(scalar(core), mine, theirs)
    outer_grad = by_core(pair, across)
    fresh_momentum = outer_beta * outer_momentum + outer_grad
    fresh_params = global_params - outer_rate * (outer_grad + outer_beta * fresh_momentum)
    return (fresh_params, fresh_momentum, next_keys)


def solution(mesh):
    finer = Mesh(mesh.devices.reshape(SIZES), AXES)
    everything = REP + FSDP
    return jax.shard_map(
        body,
        mesh=finer,
        in_specs=(
            P(everything, None),
            P(everything, None),
            P(everything, None),
            P(everything, None),
            P(everything, None),
            P(FSDP, None),
            P(REP, FSDP, None),
            P(FSDP, None),
            P(everything, None),
        ),
        out_specs=(P(FSDP, None), P(FSDP, None), P(everything, None)),
        check_vma=False,
    )
```
